32 devices in a mesh: head: 4 (over x, core), inner: 2 (over y), outer: 4 (over z).
Axes of the slice: x: 2, y: 2, z: 4, core: 2. Of those that a mesh axis runs over, the one named last changes fastest.
Arguments:
- rotated_asking_matrix: bfloat16 [4096, 32, 128], P(('head', 'inner', 'outer')), may hold values from -12 to 12
- rotated_lookup_matrix: bfloat16 [4096, 8, 128], P(('head', 'inner', 'outer')), may hold values from -6 to 6
- content_matrix: bfloat16 [4096, 8, 128], P(('head', 'inner', 'outer')), may hold values from -6 to 6
Outputs:
- attended: bfloat16 [4096, 32, 128], P(('head', 'inner', 'outer'))
The draws below stay inside these ranges and needn't reach their ends.
All inputs are finite; a program needn't handle non-finite values.
Results may differ from the reference program's by a relative error of at most 0.001.
Values may be sent and summed in bfloat16 or wider, within the bound.
A program may use at most 64 MiB of HBM per device.

```python
import jax
import jax.numpy as jnp
from jax import lax

ASKER_COUNT = 32
SHARED_ATTENDER_COUNT = 8
HEAD_WIDTH = 128
LOCAL_TOKENS = 128
SHARING_FACTOR = 4
TOTAL_TOKENS = 4096


def shard_levels(key, shape, pieces, low, high):
    factor_of = 1.0
    for dim, parts in pieces:
        draws = jax.random.uniform(jax.random.fold_in(jax.random.fold_in(key, 6), dim), (parts,), jnp.float32, low / len(pieces), high / len(pieces))
        factor_of = factor_of * jnp.repeat(jnp.exp(draws), shape[dim] // parts).reshape((-1,) + (1,) * (len(shape) - 1 - dim))
    return factor_of


def normal_values(stream_key, dims, width, reach, split=(), kind=jnp.bfloat16):
    array = jax.random.normal(stream_key, dims, jnp.float32) * width
    if len(split) > 0:
        array = shard_levels(stream_key, dims, split, -0.22, 0.18) * array
    return jnp.clip(array, min=-reach, max=reach).astype(kind)


def setup_inputs(seed: int = 0) -> dict:
    seeds = jax.random.split(jax.random.key(seed), 4)
    return {
        "rotated_asking_matrix": normal_values(seeds[0], (TOTAL_TOKENS, ASKER_COUNT, HEAD_WIDTH), 3.0, 12.0, ((0, 32),)),
        "rotated_lookup_matrix": normal_values(seeds[1], (TOTAL_TOKENS, SHARED_ATTENDER_COUNT, HEAD_WIDTH), 1.0, 6.0, ((0, 32),)),
        "content_matrix": normal_values(seeds[2], (TOTAL_TOKENS, SHARED_ATTENDER_COUNT, HEAD_WIDTH), 1.0, 6.0, ((0, 32),)),
    }


def reference(rotated_asking_matrix, rotated_lookup_matrix, content_matrix):
    number_of_segments = TOTAL_TOKENS // LOCAL_TOKENS
    asking_vectors = rotated_asking_matrix.astype(jnp.float32).reshape(number_of_segments, LOCAL_TOKENS, SHARED_ATTENDER_COUNT, SHARING_FACTOR, HEAD_WIDTH)
    key_float = rotated_lookup_matrix.astype(jnp.float32)
    value_float = content_matrix.astype(jnp.float32)
    key_pos = jnp.arange(TOTAL_TOKENS, dtype=jnp.int32)
    score_scale = 1.0 / (HEAD_WIDTH ** 0.5)

    def one_block(inputs):
        block_id, query_block = inputs
        query_pos = block_id * LOCAL_TOKENS + jnp.arange(LOCAL_TOKENS, dtype=jnp.int32)
        scores = jnp.einsum("tkgd,skd->kgts", query_block, key_float, precision=lax.Precision.HIGHEST) * score_scale
        allowed = key_pos[None, :] <= query_pos[:, None]
        scores = jnp.where(allowed, scores, -1e30)
        top = jnp.max(scores, axis=-1, keepdims=True)
        weights = jnp.where(allowed, jnp.exp(scores - top), 0.0)
        total = jnp.sum(weights, axis=-1)
        mixed = jnp.einsum("kgts,skd->kgtd", weights, value_float, precision=lax.Precision.HIGHEST)
        result = (mixed / total[..., None]).astype(jnp.bfloat16)
        return result.transpose(2, 0, 1, 3).reshape(LOCAL_TOKENS, ASKER_COUNT, HEAD_WIDTH)

    blocks = lax.map(one_block, (jnp.arange(number_of_segments, dtype=jnp.int32), asking_vectors))
    return blocks.reshape(TOTAL_TOKENS, ASKER_COUNT, HEAD_WIDTH)
```

```python
import functools
import math

import jax
import jax.numpy as jnp
from jax import lax
from jax.experimental import pallas as pl
from jax.experimental.pallas import tpu as pltpu
from jax.sharding import PartitionSpec as P

MESH = pl.DeviceIdType.MESH


def kernel(sizes, q_ref, kv_ref, out_ref, q_buf, kv_buf, o_buf, m_ref, acc_ref,
           q_send, q_recv, kv_send, kv_recv, up_send, down_send, o_send, o_recv):
    head_n, inner_n, outer_n, split, members, planes, block, group, dim = sizes
    rest = inner_n // split
    wide = group * dim
    pair = 2 * dim
    rows = group * block
    keys = planes * block
    head = lax.axis_index("head")
    inner = lax.axis_index("inner")
    outer = lax.axis_index("outer")
    me = head * split + inner // rest
    plane = (inner % rest) * outer_n + outer

    def member_id(m):
        return (m // split, (m % split) * rest + inner % rest, outer)

    def plane_id(p):
        return (head, (inner // rest) * rest + p // outer_n, p % outer_n)

    def lanes(index, width):
        return pl.ds(pl.multiple_of(index * width, dim), width)

    def slot(r, p):
        return kv_buf.at[pl.ds(pl.multiple_of((r * planes + p) * block, block), block), :]

    def kv_copy(j):
        to = (me + j) % members
        return pltpu.make_async_remote_copy(
            src_ref=kv_ref.at[:, lanes(to, pair)], dst_ref=slot(me, plane),
            send_sem=kv_send.at[j], recv_sem=kv_recv.at[me, plane],
            device_id=member_id(to), device_id_type=MESH)

    def q_copy(j):
        to = (me + j) % members
        return pltpu.make_async_remote_copy(
            src_ref=q_ref.at[:, lanes(to, wide)], dst_ref=q_buf.at[me],
            send_sem=q_send.at[j], recv_sem=q_recv.at[me],
            device_id=member_id(to), device_id_type=MESH)

    def pass_up(r, p):
        return pltpu.make_async_remote_copy(
            src_ref=slot(r, p), dst_ref=slot(r, p),
            send_sem=up_send.at[r, p], recv_sem=kv_recv.at[r, p],
            device_id=plane_id(plane + 1), device_id_type=MESH)

    def pass_down(r, p):
        return pltpu.make_async_remote_copy(
            src_ref=slot(r, p), dst_ref=slot(r, p),
            send_sem=down_send.at[r, p], recv_sem=kv_recv.at[r, p],
            device_id=plane_id(plane - 1), device_id_type=MESH)

    def out_copy(r):
        return pltpu.make_async_remote_copy(
            src_ref=o_buf.at[r], dst_ref=out_ref.at[:, lanes(me, wide)],
            send_sem=o_send.at[r], recv_sem=o_recv.at[me],
            device_id=member_id(r), device_id_type=MESH)

    def arrived(ref, sem):
        pltpu.make_async_copy(ref, ref, sem).wait()

    has_up = plane + 1 < planes
    has_down = plane > 0

    barrier = pltpu.get_barrier_semaphore()
    for j in range(1, members):
        pl.semaphore_signal(barrier, inc=1, device_id=member_id((me + j) % members),
                            device_id_type=MESH)

    @pl.when(has_up)
    def _():
        pl.semaphore_signal(barrier, inc=1, device_id=plane_id(plane + 1), device_id_type=MESH)

    @pl.when(has_down)
    def _():
        pl.semaphore_signal(barrier, inc=1, device_id=plane_id(plane - 1), device_id_type=MESH)

    pl.semaphore_wait(barrier, members - 1 + has_up.astype(jnp.int32) + has_down.astype(jnp.int32))

    for j in range(1, members):
        kv_copy(j).start()
    own_kv = pltpu.make_async_copy(
        kv_ref.at[:, lanes(me, pair)], slot(me, plane), kv_recv.at[me, plane])
    own_kv.start()
    for j in range(1, members):
        q_copy(j).start()
    own_q = pltpu.make_async_copy(q_ref.at[:, lanes(me, wide)], q_buf.at[me], q_recv.at[me])
    own_q.start()

    def gather(r, level):
        if level == 0:
            arrived(slot(r, plane), kv_recv.at[r, plane])

            @pl.when(has_up)
            def _():
                pass_up(r, plane).start()

            @pl.when(has_down)
            def _():
                pass_down(r, plane).start()
            return

        @pl.when(plane >= level)
        def _():
            p = plane - level
            arrived(slot(r, p), kv_recv.at[r, p])

            @pl.when(has_up)
            def _():
                pass_up(r, p).start()

        @pl.when(plane + level < planes)
        def _():
            p = plane + level
            arrived(slot(r, p), kv_recv.at[r, p])

            @pl.when(has_down)
            def _():
                pass_down(r, p).start()

    def gather_all(r):
        for level in range(planes):
            gather(r, level)

    factor = math.log2(math.e) / math.sqrt(dim)

    def absorb(r, c, masked):
        q = jnp.concatenate(
            [q_buf[r, :, g * dim:(g + 1) * dim] for g in range(group)], axis=0)
        kv = kv_buf[pl.ds(pl.multiple_of(c * keys, keys), keys), :]
        scores = lax.dot_general(q, kv[:, :dim], (((1,), (1,)), ((), ())),
                                 preferred_element_type=jnp.float32)
        if masked:
            t = lax.broadcasted_iota(jnp.int32, (block, keys), 0) + plane * block
            s = lax.broadcasted_iota(jnp.int32, (block, keys), 1)
            allowed = jnp.concatenate([s - t] * group, axis=0) <= 0
            scores = jnp.where(allowed, scores, -1e30)
        old = m_ref[...]
        new = jnp.maximum(old, jnp.max(scores, axis=1, keepdims=True))
        m_ref[...] = new
        fade = jnp.exp2((old - new) * factor)
        weights = jnp.exp2((scores - new[:, :1]) * factor)
        high = weights.astype(jnp.bfloat16)
        low = (weights - high.astype(jnp.float32)).astype(jnp.bfloat16)
        values = jnp.concatenate([kv[:, dim:], jnp.ones((keys, dim), jnp.bfloat16)], axis=1)
        mixed = jnp.dot(high, values, preferred_element_type=jnp.float32)
        mixed += jnp.dot(low, values, preferred_element_type=jnp.float32)
        acc_ref[...] = acc_ref[...] * jnp.concatenate([fade, fade], axis=1) + mixed

    early = min(3, members)
    for r in range(early):
        gather_all(r)

    def one_block(r, carry):
        arrived(q_buf.at[r], q_recv.at[r])
        m_ref[...] = jnp.full_like(m_ref, -1e30)
        acc_ref[...] = jnp.zeros_like(acc_ref)

        @pl.when((r < 5) & (r % 2 == 1) & ((r + 5) // 2 < members))
        def _():
            gather_all((r + 5) // 2)

        def past(c, carry):
            absorb(r, c, False)
            for level in range(planes):
                @pl.when((r >= 5) & (c == level))
                def _(level=level):
                    gather(r, level)
            return carry

        lax.fori_loop(0, r, past, 0)
        for level in range(planes):
            @pl.when((r >= 5) & (level >= r))
            def _(level=level):
                gather(r, level)
        absorb(r, r, True)
        result = (acc_ref[:, :dim] / acc_ref[:, dim:]).astype(jnp.bfloat16)
        for g in range(group):
            o_buf[r, :, g * dim:(g + 1) * dim] = result[g * block:(g + 1) * block]

        @pl.when(r != me)
        def _():
            out_copy(r).start()

        @pl.when(r == me)
        def _():
            pltpu.make_async_copy(o_buf.at[r], out_ref.at[:, lanes(me, wide)],
                                  o_recv.at[me]).start()
        return carry

    lax.fori_loop(0, members, one_block, 0)

    for j in range(1, members):
        kv_copy(j).wait_send()
        q_copy(j).wait_send()

    def finish(r, carry):
        for p in range(planes):
            @pl.when(has_up & (p <= plane))
            def _(p=p):
                pass_up(r, p).wait_send()

            @pl.when(has_down & (p >= plane))
            def _(p=p):
                pass_down(r, p).wait_send()

        @pl.when(r != me)
        def _():
            out_copy(r).wait_send()

        arrived(out_ref.at[:, lanes(r, wide)], o_recv.at[r])
        return carry

    lax.fori_loop(0, members, finish, 0)


def shards(head_n, inner_n, outer_n, q, k, v):
    block, heads, dim = q.shape
    kv_heads = k.shape[1]
    split = kv_heads // head_n
    assert split * head_n == kv_heads and inner_n % split == 0
    members = kv_heads
    planes = (inner_n // split) * outer_n
    group = heads // kv_heads
    sizes = (head_n, inner_n, outer_n, split, members, planes, block, group, dim)
    rows = group * block
    tokens = members * planes * block
    wide = group * dim
    q2 = q.reshape(block, heads * dim)
    kv2 = jnp.stack([k, v], axis=2).reshape(block, kv_heads * 2 * dim)
    dma = pltpu.SemaphoreType.DMA
    pairs = tokens * rows * planes * members // (2 * members * planes) * members
    out = pl.pallas_call(
        functools.partial(kernel, sizes),
        out_shape=jax.ShapeDtypeStruct((block, heads * dim), jnp.bfloat16),
        in_specs=[pl.BlockSpec(memory_space=pltpu.VMEM)] * 2,
        out_specs=pl.BlockSpec(memory_space=pltpu.VMEM),
        scratch_shapes=[
            pltpu.VMEM((members, block, wide), jnp.bfloat16),
            pltpu.VMEM((tokens, 2 * dim), jnp.bfloat16),
            pltpu.VMEM((members, block, wide), jnp.bfloat16),
            pltpu.VMEM((rows, dim), jnp.float32),
            pltpu.VMEM((rows, 2 * dim), jnp.float32),
            dma((members,)), dma((members,)),
            dma((members,)), dma((members, planes)),
            dma((members, planes)), dma((members, planes)),
            dma((members,)), dma((members,)),
        ],
        compiler_params=pltpu.CompilerParams(
            collective_id=0, has_side_effects=True, vmem_limit_bytes=60 * 1024 * 1024),
        cost_estimate=pl.CostEstimate(
            flops=6 * pairs * dim, bytes_accessed=4 * tokens * dim, transcendentals=pairs),
    )(q2, kv2)
    return out.reshape(block, heads, dim)


def solution(mesh):
    placed = P(("head", "inner", "outer"), None, None)
    sizes = [mesh.shape[name] for name in ("head", "inner", "outer")]
    return jax.shard_map(
        functools.partial(shards, *sizes),
        mesh=mesh,
        in_specs=(placed, placed, placed),
        out_specs=placed,
        check_vma=False,
    )
```

```python
import functools
import math

import jax
import jax.numpy as jnp
from jax import lax
from jax.experimental import pallas as pl
from jax.experimental.pallas import tpu as pltpu
from jax.sharding import PartitionSpec as P

MESH = pl.DeviceIdType.MESH


def kernel(sizes, q_ref, kv_ref, out_ref, q_buf, kv_buf, o_buf, m_ref, acc_ref,
           q_send, q_recv, kv_send, kv_recv, up_send, down_send, o_send, o_recv):
    head_n, inner_n, outer_n, split, members, planes, block, group, dim = sizes
    rest = inner_n // split
    wide = group * dim
    pair = 2 * dim
    rows = group * block
    keys = planes * block
    head = lax.axis_index("head")
    inner = lax.axis_index("inner")
    outer = lax.axis_index("outer")
    me = head * split + inner // rest
    plane = (inner % rest) * outer_n + outer

    def member_id(m):
        return (m // split, (m % split) * rest + inner % rest, outer)

    def plane_id(p):
        return (head, (inner // rest) * rest + p // outer_n, p % outer_n)

    def lanes(index, width):
        return pl.ds(pl.multiple_of(index * width, dim), width)

    def slot(r, p):
        return kv_buf.at[pl.ds(pl.multiple_of((r * planes + p) * block, block), block), :]

    def kv_copy(j):
        to = (me + j) % members
        return pltpu.make_async_remote_copy(
            src_ref=kv_ref.at[:, lanes(to, pair)], dst_ref=slot(me, plane),
            send_sem=kv_send.at[j], recv_sem=kv_recv.at[me, plane],
            device_id=member_id(to), device_id_type=MESH)

    def q_copy(j):
        to = (me + j) % members
        return pltpu.make_async_remote_copy(
            src_ref=q_ref.at[:, lanes(to, wide)], dst_ref=q_buf.at[me],
            send_sem=q_send.at[j], recv_sem=q_recv.at[me],
            device_id=member_id(to), device_id_type=MESH)

    def pass_up(r, p):
        return pltpu.make_async_remote_copy(
            src_ref=slot(r, p), dst_ref=slot(r, p),
            send_sem=up_send.at[r, p], recv_sem=kv_recv.at[r, p],
            device_id=plane_id(plane + 1), device_id_type=MESH)

    def pass_down(r, p):
        return pltpu.make_async_remote_copy(
            src_ref=slot(r, p), dst_ref=slot(r, p),
            send_sem=down_send.at[r, p], recv_sem=kv_recv.at[r, p],
            device_id=plane_id(plane - 1), device_id_type=MESH)

    def out_copy(r):
        return pltpu.make_async_remote_copy(
            src_ref=o_buf.at[r], dst_ref=out_ref.at[:, lanes(me, wide)],
            send_sem=o_send.at[r], recv_sem=o_recv.at[me],
            device_id=member_id(r), device_id_type=MESH)

    def arrived(ref, sem):
        pltpu.make_async_copy(ref, ref, sem).wait()

    has_up = plane + 1 < planes
    has_down = plane > 0

    barrier = pltpu.get_barrier_semaphore()
    for j in range(1, members):
        pl.semaphore_signal(barrier, inc=1, device_id=member_id((me + j) % members),
                            device_id_type=MESH)

    @pl.when(has_up)
    def _():
        pl.semaphore_signal(barrier, inc=1, device_id=plane_id(plane + 1), device_id_type=MESH)

    @pl.when(has_down)
    def _():
        pl.semaphore_signal(barrier, inc=1, device_id=plane_id(plane - 1), device_id_type=MESH)

    pl.semaphore_wait(barrier, members - 1 + has_up.astype(jnp.int32) + has_down.astype(jnp.int32))

    for j in range(1, members):
        kv_copy(j).start()
    own_kv = pltpu.make_async_copy(
        kv_ref.at[:, lanes(me, pair)], slot(me, plane), kv_recv.at[me, plane])
    own_kv.start()
    for j in range(1, members):
        q_copy(j).start()
    own_q = pltpu.make_async_copy(q_ref.at[:, lanes(me, wide)], q_buf.at[me], q_recv.at[me])
    own_q.start()

    def gather(r, level):
        if level == 0:
            arrived(slot(r, plane), kv_recv.at[r, plane])

            @pl.when(has_up)
            def _():
                pass_up(r, plane).start()

            @pl.when(has_down)
            def _():
                pass_down(r, plane).start()
            return

        @pl.when(plane >= level)
        def _():
            p = plane - level
            arrived(slot(r, p), kv_recv.at[r, p])

            @pl.when(has_up)
            def _():
                pass_up(r, p).start()

        @pl.when(plane + level < planes)
        def _():
            p = plane + level
            arrived(slot(r, p), kv_recv.at[r, p])

            @pl.when(has_down)
            def _():
                pass_down(r, p).start()

    def advance(t, part):
        r = t + 1 if part == 0 else t - part

        @pl.when((r >= 0) & (r < members))
        def _():
            gather(r, part)

    factor = math.log2(math.e) / math.sqrt(dim)

    def absorb(r, c, masked):
        kv = kv_buf[pl.ds(pl.multiple_of(c * keys, keys), keys), :]
        values = jnp.concatenate(
            [kv[:, dim:].T, jnp.ones((16, keys), jnp.bfloat16)], axis=0)
        if masked:
            t = lax.broadcasted_iota(jnp.int32, (keys, block), 1) + plane * block
            s = lax.broadcasted_iota(jnp.int32, (keys, block), 0)
            allowed = s <= t
        q = jnp.concatenate([q_buf[r, :, g * dim:(g + 1) * dim] for g in range(group)], axis=0)
        scores = lax.dot_general(kv[:, :dim], q, (((1,), (1,)), ((), ())),
                                 preferred_element_type=jnp.float32)
        if masked:
            scores = jnp.where(jnp.concatenate([allowed] * group, axis=1), scores, -1e30)
        old = m_ref[:1, :]
        new = jnp.maximum(old, jnp.max(scores, axis=0, keepdims=True))
        m_ref[:1, :] = new
        fade = jnp.exp2((old - new) * factor)
        weights = jnp.exp2((scores - new) * factor)
        high = weights.astype(jnp.bfloat16)
        low = (weights - high.astype(jnp.float32)).astype(jnp.bfloat16)
        mixed = jnp.dot(values, high, preferred_element_type=jnp.float32)
        mixed += jnp.dot(values, low, preferred_element_type=jnp.float32)
        acc_ref[...] = acc_ref[...] * fade + mixed

    gather(0, 0)
    for t in range(planes - 1):
        for part in range(t + 1):
            advance(jnp.int32(t), part)

    def one_block(r, carry):
        arrived(q_buf.at[r], q_recv.at[r])
        m_ref[...] = jnp.full_like(m_ref, -1e30)
        acc_ref[...] = jnp.zeros_like(acc_ref)

        def past(c, carry):
            absorb(r, c, False)
            for level in range(planes):
                @pl.when(c == level)
                def _(level=level):
                    advance(r + planes - 1, level)
            return carry

        lax.fori_loop(0, r, past, 0)
        for level in range(planes):
            @pl.when(level >= r)
            def _(level=level):
                advance(r + planes - 1, level)
        absorb(r, r, True)
        for g in range(group):
            at = pl.ds(g * block, block)
            result = acc_ref[:dim, at] / acc_ref[dim:dim + 1, at]
            o_buf[r, :, g * dim:(g + 1) * dim] = result.T.astype(jnp.bfloat16)

        @pl.when(r != me)
        def _():
            out_copy(r).start()

        @pl.when(r == me)
        def _():
            pltpu.make_async_copy(o_buf.at[r], out_ref.at[:, lanes(me, wide)],
                                  o_recv.at[me]).start()
        return carry

    lax.fori_loop(0, members, one_block, 0)

    for j in range(1, members):
        kv_copy(j).wait_send()
        q_copy(j).wait_send()

    def finish(r, carry):
        for p in range(planes):
            @pl.when(has_up & (p <= plane))
            def _(p=p):
                pass_up(r, p).wait_send()

            @pl.when(has_down & (p >= plane))
            def _(p=p):
                pass_down(r, p).wait_send()

        @pl.when(r != me)
        def _():
            out_copy(r).wait_send()

        arrived(out_ref.at[:, lanes(r, wide)], o_recv.at[r])
        return carry

    lax.fori_loop(0, members, finish, 0)


def shards(head_n, inner_n, outer_n, q, k, v):
    block, heads, dim = q.shape
    kv_heads = k.shape[1]
    split = kv_heads // head_n
    assert split * head_n == kv_heads and inner_n % split == 0
    members = kv_heads
    planes = (inner_n // split) * outer_n
    group = heads // kv_heads
    sizes = (head_n, inner_n, outer_n, split, members, planes, block, group, dim)
    rows = group * block
    tokens = members * planes * block
    wide = group * dim
    q2 = q.reshape(block, heads * dim)
    kv2 = jnp.stack([k, v], axis=2).reshape(block, kv_heads * 2 * dim)
    dma = pltpu.SemaphoreType.DMA
    pairs = tokens * rows * planes * members // (2 * members * planes) * members
    out = pl.pallas_call(
        functools.partial(kernel, sizes),
        out_shape=jax.ShapeDtypeStruct((block, heads * dim), jnp.bfloat16),
        in_specs=[pl.BlockSpec(memory_space=pltpu.VMEM)] * 2,
        out_specs=pl.BlockSpec(memory_space=pltpu.VMEM),
        scratch_shapes=[
            pltpu.VMEM((members, block, wide), jnp.bfloat16),
            pltpu.VMEM((tokens, 2 * dim), jnp.bfloat16),
            pltpu.VMEM((members, block, wide), jnp.bfloat16),
            pltpu.VMEM((8, rows), jnp.float32),
            pltpu.VMEM((dim + 16, rows), jnp.float32),
            dma((members,)), dma((members,)),
            dma((members,)), dma((members, planes)),
            dma((members, planes)), dma((members, planes)),
            dma((members,)), dma((members,)),
        ],
        compiler_params=pltpu.CompilerParams(
            collective_id=0, has_side_effects=True, vmem_limit_bytes=60 * 1024 * 1024),
        cost_estimate=pl.CostEstimate(
            flops=6 * pairs * dim, bytes_accessed=4 * tokens * dim, transcendentals=pairs),
    )(q2, kv2)
    return out.reshape(block, heads, dim)


def solution(mesh):
    placed = P(("head", "inner", "outer"), None, None)
    sizes = [mesh.shape[name] for name in ("head", "inner", "outer")]
    return jax.shard_map(
        functools.partial(shards, *sizes),
        mesh=mesh,
        in_specs=(placed, placed, placed),
        out_specs=placed,
        check_vma=False,
    )
```

```python
import functools
import math

import jax
import jax.numpy as jnp
from jax import lax
from jax.experimental import pallas as pl
from jax.experimental.pallas import tpu as pltpu
from jax.sharding import PartitionSpec as P

MESH = pl.DeviceIdType.MESH


def kernel(sizes, q_ref, k_ref, v_ref, out_ref, q_buf, kv_buf, o_buf, m_ref, acc_ref,
           q_send, q_recv, k_send, v_send, k_recv, v_recv, kv_recv, up_send, down_send, o_send, o_recv):
    head_n, inner_n, outer_n, split, members, planes, block, group, dim = sizes
    rest = inner_n // split
    wide = group * dim
    rows = group * block
    keys = planes * block
    head = lax.axis_index("head")
    inner = lax.axis_index("inner")
    outer = lax.axis_index("outer")
    me = head * split + inner // rest
    plane = (inner % rest) * outer_n + outer

    def member_id(m):
        return (m // split, (m % split) * rest + inner % rest, outer)

    def plane_id(p):
        return (head, (inner // rest) * rest + p // outer_n, p % outer_n)

    def lanes(index, width):
        return pl.ds(pl.multiple_of(index * width, dim), width)

    def slot(r, p):
        return kv_buf.at[r * planes + p]

    def k_half(r, p):
        return kv_buf.at[r * planes + p, :, pl.ds(0, dim)]

    def v_half(r, p):
        return kv_buf.at[r * planes + p, :, pl.ds(dim, block)]

    def k_copy(j):
        to = (me + j) % members
        return pltpu.make_async_remote_copy(
            src_ref=k_ref.at[:, lanes(to, dim)], dst_ref=k_half(me, plane),
            send_sem=k_send.at[j], recv_sem=k_recv.at[me],
            device_id=member_id(to), device_id_type=MESH)

    def v_copy(j):
        to = (me + j) % members
        return pltpu.make_async_remote_copy(
            src_ref=v_ref.at[:, lanes(to, block)], dst_ref=v_half(me, plane),
            send_sem=v_send.at[j], recv_sem=v_recv.at[me],
            device_id=member_id(to), device_id_type=MESH)

    def q_copy(j):
        to = (me + j) % members
        return pltpu.make_async_remote_copy(
            src_ref=q_ref.at[:, lanes(to, wide)], dst_ref=q_buf.at[me],
            send_sem=q_send.at[j], recv_sem=q_recv.at[me],
            device_id=member_id(to), device_id_type=MESH)

    def pass_up(r, p):
        return pltpu.make_async_remote_copy(
            src_ref=slot(r, p), dst_ref=slot(r, p),
            send_sem=up_send.at[r, p], recv_sem=kv_recv.at[r, p],
            device_id=plane_id(plane + 1), device_id_type=MESH)

    def pass_down(r, p):
        return pltpu.make_async_remote_copy(
            src_ref=slot(r, p), dst_ref=slot(r, p),
            send_sem=down_send.at[r, p], recv_sem=kv_recv.at[r, p],
            device_id=plane_id(plane - 1), device_id_type=MESH)

    def out_copy(r):
        return pltpu.make_async_remote_copy(
            src_ref=o_buf.at[r], dst_ref=out_ref.at[:, lanes(me, wide)],
            send_sem=o_send.at[r], recv_sem=o_recv.at[me],
            device_id=member_id(r), device_id_type=MESH)

    def arrived(ref, sem):
        pltpu.make_async_copy(ref, ref, sem).wait()

    has_up = plane + 1 < planes
    has_down = plane > 0

    for p in range(1, planes):
        @pl.when(p > plane)
        def _(p=p):
            kv_buf[(members - 1) * planes + p] = jnp.zeros((block, dim + block), jnp.bfloat16)

    barrier = pltpu.get_barrier_semaphore()
    for j in range(1, members):
        pl.semaphore_signal(barrier, inc=1, device_id=member_id((me + j) % members),
                            device_id_type=MESH)

    @pl.when(has_up)
    def _():
        pl.semaphore_signal(barrier, inc=1, device_id=plane_id(plane + 1), device_id_type=MESH)

    @pl.when(has_down)
    def _():
        pl.semaphore_signal(barrier, inc=1, device_id=plane_id(plane - 1), device_id_type=MESH)

    pl.semaphore_wait(barrier, members - 1 + has_up.astype(jnp.int32) + has_down.astype(jnp.int32))

    for j in range(1, members):
        k_copy(j).start()
        v_copy(j).start()
    own_k = pltpu.make_async_copy(k_ref.at[:, lanes(me, dim)], k_half(me, plane), k_recv.at[me])
    own_k.start()
    own_v = pltpu.make_async_copy(v_ref.at[:, lanes(me, block)], v_half(me, plane), v_recv.at[me])
    own_v.start()
    for j in range(1, members):
        q_copy(j).start()
    own_q = pltpu.make_async_copy(q_ref.at[:, lanes(me, wide)], q_buf.at[me], q_recv.at[me])
    own_q.start()

    def gather(r, level):
        if level == 0:
            arrived(k_half(r, plane), k_recv.at[r])
            arrived(v_half(r, plane), v_recv.at[r])

            @pl.when(has_up)
            def _():
                pass_up(r, plane).start()

            @pl.when(has_down & (r < members - 1))
            def _():
                pass_down(r, plane).start()
            return

        @pl.when(plane >= level)
        def _():
            p = plane - level
            arrived(slot(r, p), kv_recv.at[r, p])

            @pl.when(has_up)
            def _():
                pass_up(r, p).start()

        @pl.when((plane + level < planes) & (r < members - 1))
        def _():
            p = plane + level
            arrived(slot(r, p), kv_recv.at[r, p])

            @pl.when(has_down)
            def _():
                pass_down(r, p).start()

    def advance(t, part):
        r = t + 1 if part == 0 else t - part

        @pl.when((r >= 0) & (r < members))
        def _():
            gather(r, part)

    factor = math.log2(math.e) / math.sqrt(dim)

    def absorb(r, c, masked):
        parts = [kv_buf[c * planes + p] for p in range(planes)]
        looked = jnp.concatenate([part[:, :dim] for part in parts], axis=0)
        values = jnp.concatenate([part[:, dim:] for part in parts], axis=1)
        values = jnp.concatenate([values, jnp.ones((16, keys), jnp.bfloat16)], axis=0)
        if masked:
            t = lax.broadcasted_iota(jnp.int32, (keys, block), 1) + plane * block
            s = lax.broadcasted_iota(jnp.int32, (keys, block), 0)
            allowed = s <= t
        q = jnp.concatenate([q_buf[r, :, g * dim:(g + 1) * dim] for g in range(group)], axis=0)
        scores = lax.dot_general(looked, q, (((1,), (1,)), ((), ())),
                                 preferred_element_type=jnp.float32)
        if masked:
            scores = jnp.where(jnp.concatenate([allowed] * group, axis=1), scores, -1e30)
        old = m_ref[r, :1, :]
        new = jnp.maximum(old, jnp.max(scores, axis=0, keepdims=True))
        m_ref[r, :1, :] = new
        fade = jnp.exp2((old - new) * factor)
        weights = jnp.exp2((scores - new) * factor)
        high = weights.astype(jnp.bfloat16)
        low = (weights - high.astype(jnp.float32)).astype(jnp.bfloat16)
        mixed = jnp.dot(values, high, preferred_element_type=jnp.float32)
        mixed += jnp.dot(values, low, preferred_element_type=jnp.float32)
        acc_ref[r] = acc_ref[r] * fade + mixed

    m_ref[...] = jnp.full_like(m_ref, -1e30)
    acc_ref[...] = jnp.zeros_like(acc_ref)
    gather(0, 0)
    for t in range(planes - 1):
        for part in range(t + 1):
            advance(jnp.int32(t), part)

    half = members // 2

    def one_block(r, carry):
        @pl.when(r <= half)
        def _():
            arrived(q_buf.at[r], q_recv.at[r])

        ahead = jnp.where(r >= 1, jnp.maximum(members - half - r, 0), 0)
        first = jnp.maximum(r - half, 0)
        count = ahead + r - first

        def past(i, carry):
            late = i < ahead
            block_id = jnp.where(late, r + half + i, r)
            chunk = jnp.where(late, r - 1, first + i - ahead)

            @pl.when(late & (r == 1))
            def _():
                arrived(q_buf.at[block_id], q_recv.at[block_id])

            absorb(block_id, chunk, False)
            for level in range(planes):
                @pl.when(i == level)
                def _(level=level):
                    advance(r + planes - 1, level)

            return carry

        lax.fori_loop(0, count, past, 0)
        for level in range(planes):
            @pl.when(level >= count)
            def _(level=level):
                advance(r + planes - 1, level)
        absorb(r, r, True)
        for g in range(group):
            at = pl.ds(g * block, block)
            result = acc_ref[r, :dim, at] / acc_ref[r, dim:dim + 1, at]
            o_buf[r, :, g * dim:(g + 1) * dim] = result.T.astype(jnp.bfloat16)

        @pl.when(r != me)
        def _():
            out_copy(r).start()

        @pl.when(r == me)
        def _():
            pltpu.make_async_copy(o_buf.at[r], out_ref.at[:, lanes(me, wide)],
                                  o_recv.at[me]).start()
        return carry

    lax.fori_loop(0, members, one_block, 0)

    for j in range(1, members):
        k_copy(j).wait_send()
        v_copy(j).wait_send()
        q_copy(j).wait_send()

    def finish(r, carry):
        for p in range(planes):
            @pl.when(has_up & (p <= plane))
            def _(p=p):
                pass_up(r, p).wait_send()

            @pl.when(has_down & (p >= plane) & (r < members - 1))
            def _(p=p):
                pass_down(r, p).wait_send()

        @pl.when(r != me)
        def _():
            out_copy(r).wait_send()

        arrived(out_ref.at[:, lanes(r, wide)], o_recv.at[r])
        return carry

    lax.fori_loop(0, members, finish, 0)


def shards(head_n, inner_n, outer_n, q, k, v):
    block, heads, dim = q.shape
    kv_heads = k.shape[1]
    split = kv_heads // head_n
    assert split * head_n == kv_heads and inner_n % split == 0
    members = kv_heads
    planes = (inner_n // split) * outer_n
    group = heads // kv_heads
    sizes = (head_n, inner_n, outer_n, split, members, planes, block, group, dim)
    rows = group * block
    tokens = members * planes * block
    wide = group * dim
    q2 = q.reshape(block, heads * dim)
    k2 = k.reshape(block, kv_heads * dim)
    v2 = v.transpose(2, 1, 0).reshape(dim, kv_heads * block)
    assert dim == block
    dma = pltpu.SemaphoreType.DMA
    pairs = tokens * rows * planes * members // (2 * members * planes) * members
    out = pl.pallas_call(
        functools.partial(kernel, sizes),
        out_shape=jax.ShapeDtypeStruct((block, heads * dim), jnp.bfloat16),
        in_specs=[pl.BlockSpec(memory_space=pltpu.VMEM)] * 3,
        out_specs=pl.BlockSpec(memory_space=pltpu.VMEM),
        scratch_shapes=[
            pltpu.VMEM((members, block, wide), jnp.bfloat16),
            pltpu.VMEM((members * planes, block, dim + block), jnp.bfloat16),
            pltpu.VMEM((members, block, wide), jnp.bfloat16),
            pltpu.VMEM((members, 8, rows), jnp.float32),
            pltpu.VMEM((members, dim + 16, rows), jnp.float32),
            dma((members,)), dma((members,)),
            dma((members,)), dma((members,)), dma((members,)), dma((members,)),
            dma((members, planes)), dma((members, planes)), dma((members, planes)),
            dma((members,)), dma((members,)),
        ],
        compiler_params=pltpu.CompilerParams(
            collective_id=0, has_side_effects=True, vmem_limit_bytes=60 * 1024 * 1024),
        cost_estimate=pl.CostEstimate(
            flops=6 * pairs * dim, bytes_accessed=4 * tokens * dim, transcendentals=pairs),
    )(q2, k2, v2)
    return out.reshape(block, heads, dim)


def solution(mesh):
    placed = P(("head", "inner", "outer"), None, None)
    sizes = [mesh.shape[name] for name in ("head", "inner", "outer")]
    return jax.shard_map(
        functools.partial(shards, *sizes),
        mesh=mesh,
        in_specs=(placed, placed, placed),
        out_specs=placed,
        check_vma=False,
    )
```

```python
import functools
import math

import jax
import jax.numpy as jnp
from jax import lax
from jax.experimental import pallas as pl
from jax.experimental.pallas import tpu as pltpu
from jax.sharding import PartitionSpec as P

MESH = pl.DeviceIdType.MESH


def kernel(sizes, q_ref, k_ref, v_ref, out_ref, q_buf, kv_buf, o_buf, m_ref, acc_ref,
           q_send, q_recv, k_send, v_send, k_recv, v_recv, kv_recv, up_send, down_send, o_send, o_recv):
    head_n, inner_n, outer_n, split, members, planes, block, group, dim = sizes
    rest = inner_n // split
    wide = group * dim
    rows = group * block
    keys = planes * block
    head = lax.axis_index("head")
    inner = lax.axis_index("inner")
    outer = lax.axis_index("outer")
    me = head * split + inner // rest
    plane = (inner % rest) * outer_n + outer

    def member_id(m):
        return (m // split, (m % split) * rest + inner % rest, outer)

    def plane_id(p):
        return (head, (inner // rest) * rest + p // outer_n, p % outer_n)

    def lanes(index, width):
        return pl.ds(pl.multiple_of(index * width, dim), width)

    def slot(r, p):
        return kv_buf.at[r * planes + p]

    def k_half(r, p):
        return kv_buf.at[r * planes + p, :, pl.ds(0, dim)]

    def v_half(r, p):
        return kv_buf.at[r * planes + p, :, pl.ds(dim, block)]

    def k_copy(j):
        to = (me + j) % members
        return pltpu.make_async_remote_copy(
            src_ref=k_ref.at[:, lanes(to, dim)], dst_ref=k_half(me, plane),
            send_sem=k_send.at[j], recv_sem=k_recv.at[me],
            device_id=member_id(to), device_id_type=MESH)

    def v_copy(j):
        to = (me + j) % members
        return pltpu.make_async_remote_copy(
            src_ref=v_ref.at[:, lanes(to, block)], dst_ref=v_half(me, plane),
            send_sem=v_send.at[j], recv_sem=v_recv.at[me],
            device_id=member_id(to), device_id_type=MESH)

    def q_copy(j):
        to = (me + j) % members
        return pltpu.make_async_remote_copy(
            src_ref=q_ref.at[:, lanes(to, wide)], dst_ref=q_buf.at[me],
            send_sem=q_send.at[j], recv_sem=q_recv.at[me],
            device_id=member_id(to), device_id_type=MESH)

    def pass_up(r, p):
        return pltpu.make_async_remote_copy(
            src_ref=slot(r, p), dst_ref=slot(r, p),
            send_sem=up_send.at[r, p], recv_sem=kv_recv.at[r, p],
            device_id=plane_id(plane + 1), device_id_type=MESH)

    def pass_down(r, p):
        return pltpu.make_async_remote_copy(
            src_ref=slot(r, p), dst_ref=slot(r, p),
            send_sem=down_send.at[r, p], recv_sem=kv_recv.at[r, p],
            device_id=plane_id(plane - 1), device_id_type=MESH)

    def out_copy(r):
        return pltpu.make_async_remote_copy(
            src_ref=o_buf.at[r], dst_ref=out_ref.at[:, lanes(me, wide)],
            send_sem=o_send.at[r], recv_sem=o_recv.at[me],
            device_id=member_id(r), device_id_type=MESH)

    def arrived(ref, sem):
        pltpu.make_async_copy(ref, ref, sem).wait()

    has_up = plane + 1 < planes
    has_down = plane > 0

    for p in range(1, planes):
        @pl.when(p > plane)
        def _(p=p):
            kv_buf[(members - 1) * planes + p] = jnp.zeros((block, dim + block), jnp.bfloat16)

    barrier = pltpu.get_barrier_semaphore()
    for j in range(1, members):
        pl.semaphore_signal(barrier, inc=1, device_id=member_id((me + j) % members),
                            device_id_type=MESH)

    @pl.when(has_up)
    def _():
        pl.semaphore_signal(barrier, inc=1, device_id=plane_id(plane + 1), device_id_type=MESH)

    @pl.when(has_down)
    def _():
        pl.semaphore_signal(barrier, inc=1, device_id=plane_id(plane - 1), device_id_type=MESH)

    pl.semaphore_wait(barrier, members - 1 + has_up.astype(jnp.int32) + has_down.astype(jnp.int32))

    for j in range(1, members):
        k_copy(j).start()
        v_copy(j).start()
    own_k = pltpu.make_async_copy(k_ref.at[:, lanes(me, dim)], k_half(me, plane), k_recv.at[me])
    own_k.start()
    own_v = pltpu.make_async_copy(v_ref.at[:, lanes(me, block)], v_half(me, plane), v_recv.at[me])
    own_v.start()
    for j in range(1, members):
        q_copy(j).start()
    own_q = pltpu.make_async_copy(q_ref.at[:, lanes(me, wide)], q_buf.at[me], q_recv.at[me])
    own_q.start()

    def gather(r, level):
        if level == 0:
            arrived(k_half(r, plane), k_recv.at[r])
            arrived(v_half(r, plane), v_recv.at[r])

            @pl.when(has_up)
            def _():
                pass_up(r, plane).start()

            @pl.when(has_down & (r < members - 1))
            def _():
                pass_down(r, plane).start()
            return

        @pl.when(plane >= level)
        def _():
            p = plane - level
            arrived(slot(r, p), kv_recv.at[r, p])

            @pl.when(has_up)
            def _():
                pass_up(r, p).start()

        @pl.when((plane + level < planes) & (r < members - 1))
        def _():
            p = plane + level
            arrived(slot(r, p), kv_recv.at[r, p])

            @pl.when(has_down)
            def _():
                pass_down(r, p).start()

    def advance(t, part):
        r = t + 1 if part == 0 else t - part

        @pl.when((r >= 0) & (r < members))
        def _():
            gather(r, part)

    factor = math.log2(math.e) / math.sqrt(dim)

    def absorb(r, c, masked):
        parts = [kv_buf[c * planes + p] for p in range(planes)]
        looked = jnp.concatenate([part[:, :dim] for part in parts], axis=0)
        values = jnp.concatenate([part[:, dim:] for part in parts], axis=1)
        values = jnp.concatenate([values, jnp.ones((16, keys), jnp.bfloat16)], axis=0)
        if masked:
            t = lax.broadcasted_iota(jnp.int32, (keys, block), 1) + plane * block
            s = lax.broadcasted_iota(jnp.int32, (keys, block), 0)
            allowed = s <= t
        q = jnp.concatenate([q_buf[r, :, g * dim:(g + 1) * dim] for g in range(group)], axis=0)
        scores = lax.dot_general(looked, q, (((1,), (1,)), ((), ())),
                                 preferred_element_type=jnp.float32)
        if masked:
            scores = jnp.where(jnp.concatenate([allowed] * group, axis=1), scores, -1e30)
        old = m_ref[r, :1, :]
        new = jnp.maximum(old, jnp.max(scores, axis=0, keepdims=True))
        m_ref[r, :1, :] = new
        fade = jnp.exp2((old - new) * factor)
        weights = jnp.exp2((scores - new) * factor)
        high = weights.astype(jnp.bfloat16)
        low = (weights - high.astype(jnp.float32)).astype(jnp.bfloat16)
        mixed = jnp.dot(values, high, preferred_element_type=jnp.float32)
        mixed += jnp.dot(values, low, preferred_element_type=jnp.float32)
        acc_ref[r] = acc_ref[r] * fade + mixed

    m_ref[...] = jnp.full_like(m_ref, -1e30)
    acc_ref[...] = jnp.zeros_like(acc_ref)
    gather(0, 0)
    for t in range(planes - 1):
        for part in range(t + 1):
            advance(jnp.int32(t), part)

    half = members // 2

    def one_block(r, carry):
        @pl.when(r <= half)
        def _():
            arrived(q_buf.at[r], q_recv.at[r])

        ahead = jnp.where(r >= 1, jnp.maximum(members - half - r, 0), 0)
        first = jnp.maximum(r - half, 0)
        count = ahead + r - first

        def past(i, carry):
            late = i < ahead
            block_id = jnp.where(late, r + half + i, r)
            chunk = jnp.where(late, r - 1, first + i - ahead)

            @pl.when(late & (r == 1))
            def _():
                arrived(q_buf.at[block_id], q_recv.at[block_id])

            absorb(block_id, chunk, False)
            for level in range(planes):
                @pl.when(i == level)
                def _(level=level):
                    advance(r + planes - 1, level)

            return carry

        lax.fori_loop(0, count, past, 0)
        for level in range(planes):
            @pl.when(level >= count)
            def _(level=level):
                advance(r + planes - 1, level)
        absorb(r, r, True)
        for g in range(group):
            at = pl.ds(g * block, block)
            result = acc_ref[r, :dim, at] / acc_ref[r, dim:dim + 1, at]
            o_buf[r, :, g * dim:(g + 1) * dim] = result.T.astype(jnp.bfloat16)

        @pl.when(r != me)
        def _():
            out_copy(r).start()

        @pl.when(r == me)
        def _():
            pltpu.make_async_copy(o_buf.at[r], out_ref.at[:, lanes(me, wide)],
                                  o_recv.at[me]).start()
        return carry

    lax.fori_loop(0, members, one_block, 0)

    for j in range(1, members):
        k_copy(j).wait_send()
        v_copy(j).wait_send()
        q_copy(j).wait_send()

    def finish(r, carry):
        for p in range(planes):
            @pl.when(has_up & (p <= plane))
            def _(p=p):
                pass_up(r, p).wait_send()

            @pl.when(has_down & (p >= plane) & (r < members - 1))
            def _(p=p):
                pass_down(r, p).wait_send()

        @pl.when(r != me)
        def _():
            out_copy(r).wait_send()

        arrived(out_ref.at[:, lanes(r, wide)], o_recv.at[r])
        return carry

    lax.fori_loop(0, members, finish, 0)


def shards(head_n, inner_n, outer_n, q, k, v):
    block, heads, dim = q.shape
    kv_heads = k.shape[1]
    split = kv_heads // head_n
    assert split * head_n == kv_heads and inner_n % split == 0
    members = kv_heads
    planes = (inner_n // split) * outer_n
    group = heads // kv_heads
    sizes = (head_n, inner_n, outer_n, split, members, planes, block, group, dim)
    rows = group * block
    tokens = members * planes * block
    wide = group * dim
    q2 = q.reshape(block, heads * dim)
    k2 = k.reshape(block, kv_heads * dim)
    v2 = v.transpose(2, 1, 0).reshape(dim, kv_heads * block)
    assert dim == block
    dma = pltpu.SemaphoreType.DMA
    pairs = tokens * rows * planes * members // (2 * members * planes) * members
    out = pl.pallas_call(
        functools.partial(kernel, sizes),
        out_shape=jax.ShapeDtypeStruct((block, heads * dim), jnp.bfloat16),
        in_specs=[pl.BlockSpec(memory_space=pl.ANY)] * 3,
        out_specs=pl.BlockSpec(memory_space=pltpu.VMEM),
        scratch_shapes=[
            pltpu.VMEM((members, block, wide), jnp.bfloat16),
            pltpu.VMEM((members * planes, block, dim + block), jnp.bfloat16),
            pltpu.VMEM((members, block, wide), jnp.bfloat16),
            pltpu.VMEM((members, 8, rows), jnp.float32),
            pltpu.VMEM((members, dim + 16, rows), jnp.float32),
            dma((members,)), dma((members,)),
            dma((members,)), dma((members,)), dma((members,)), dma((members,)),
            dma((members, planes)), dma((members, planes)), dma((members, planes)),
            dma((members,)), dma((members,)),
        ],
        compiler_params=pltpu.CompilerParams(
            collective_id=0, has_side_effects=True, vmem_limit_bytes=2 ** 24 + 16 * tokens * dim),
        cost_estimate=pl.CostEstimate(
            flops=6 * pairs * dim, bytes_accessed=4 * tokens * dim, transcendentals=pairs),
    )(q2, k2, v2)
    return out.reshape(block, heads, dim)


def solution(mesh):
    placed = P(("head", "inner", "outer"), None, None)
    sizes = [mesh.shape[name] for name in ("head", "inner", "outer")]
    return jax.shard_map(
        functools.partial(shards, *sizes),
        mesh=mesh,
        in_specs=(placed, placed, placed),
        out_specs=placed,
        check_vma=False,
    )
```

```python
import functools
import math

import jax
import jax.numpy as jnp
from jax import lax
from jax.experimental import pallas as pl
from jax.experimental.pallas import tpu as pltpu
from jax.sharding import PartitionSpec as P

MESH = pl.DeviceIdType.MESH


def kernel(sizes, q_ref, k_ref, v_ref, out_ref, q_buf, kv_buf, o_buf, m_ref, acc_ref,
           q_send, q_recv, k_send, v_send, k_recv, v_recv, kv_recv, up_send, down_send, o_send, o_recv):
    head_n, inner_n, outer_n, split, members, planes, block, group, dim = sizes
    rest = inner_n // split
    wide = group * dim
    rows = group * block
    keys = planes * block
    head = lax.axis_index("head")
    inner = lax.axis_index("inner")
    outer = lax.axis_index("outer")
    me = head * split + inner // rest
    plane = (inner % rest) * outer_n + outer

    def member_id(m):
        return (m // split, (m % split) * rest + inner % rest, outer)

    def plane_id(p):
        return (head, (inner // rest) * rest + p // outer_n, p % outer_n)

    def lanes(index, width):
        return pl.ds(pl.multiple_of(index * width, dim), width)

    def slot(r, p):
        return kv_buf.at[r * planes + p]

    def k_half(r, p):
        return kv_buf.at[r * planes + p, :, pl.ds(0, dim)]

    def v_half(r, p):
        return kv_buf.at[r * planes + p, :, pl.ds(dim, block)]

    def k_copy(j):
        to = (me + j) % members
        return pltpu.make_async_remote_copy(
            src_ref=k_ref.at[:, lanes(to, dim)], dst_ref=k_half(me, plane),
            send_sem=k_send.at[j], recv_sem=k_recv.at[me],
            device_id=member_id(to), device_id_type=MESH)

    def v_copy(j):
        to = (me + j) % members
        return pltpu.make_async_remote_copy(
            src_ref=v_ref.at[:, lanes(to, block)], dst_ref=v_half(me, plane),
            send_sem=v_send.at[j], recv_sem=v_recv.at[me],
            device_id=member_id(to), device_id_type=MESH)

    def q_copy(j):
        to = (me + j) % members
        return pltpu.make_async_remote_copy(
            src_ref=q_ref.at[:, lanes(to, wide)], dst_ref=q_buf.at[me],
            send_sem=q_send.at[j], recv_sem=q_recv.at[me],
            device_id=member_id(to), device_id_type=MESH)

    def pass_up(r, p):
        return pltpu.make_async_remote_copy(
            src_ref=slot(r, p), dst_ref=slot(r, p),
            send_sem=up_send.at[r, p], recv_sem=kv_recv.at[r, p],
            device_id=plane_id(plane + 1), device_id_type=MESH)

    def pass_down(r, p):
        return pltpu.make_async_remote_copy(
            src_ref=slot(r, p), dst_ref=slot(r, p),
            send_sem=down_send.at[r, p], recv_sem=kv_recv.at[r, p],
            device_id=plane_id(plane - 1), device_id_type=MESH)

    def out_copy(r):
        return pltpu.make_async_remote_copy(
            src_ref=o_buf.at[r], dst_ref=out_ref.at[:, lanes(me, wide)],
            send_sem=o_send.at[r], recv_sem=o_recv.at[me],
            device_id=member_id(r), device_id_type=MESH)

    def arrived(ref, sem):
        pltpu.make_async_copy(ref, ref, sem).wait()

    has_up = plane + 1 < planes
    has_down = plane > 0

    for p in range(1, planes):
        @pl.when(p > plane)
        def _(p=p):
            kv_buf[(members - 1) * planes + p] = jnp.zeros((block, dim + block), jnp.bfloat16)

    barrier = pltpu.get_barrier_semaphore()
    for j in range(1, members):
        pl.semaphore_signal(barrier, inc=1, device_id=member_id((me + j) % members),
                            device_id_type=MESH)

    @pl.when(has_up)
    def _():
        pl.semaphore_signal(barrier, inc=1, device_id=plane_id(plane + 1), device_id_type=MESH)

    @pl.when(has_down)
    def _():
        pl.semaphore_signal(barrier, inc=1, device_id=plane_id(plane - 1), device_id_type=MESH)

    pl.semaphore_wait(barrier, members - 1 + has_up.astype(jnp.int32) + has_down.astype(jnp.int32))

    for j in range(1, members):
        k_copy(j).start()
        v_copy(j).start()
    own_k = pltpu.make_async_copy(k_ref.at[:, lanes(me, dim)], k_half(me, plane), k_recv.at[me])
    own_k.start()
    own_v = pltpu.make_async_copy(v_ref.at[:, lanes(me, block)], v_half(me, plane), v_recv.at[me])
    own_v.start()
    for j in range(1, members):
        q_copy(j).start()
    own_q = pltpu.make_async_copy(q_ref.at[:, lanes(me, wide)], q_buf.at[me], q_recv.at[me])
    own_q.start()

    def gather(r, level):
        if level == 0:
            arrived(k_half(r, plane), k_recv.at[r])
            arrived(v_half(r, plane), v_recv.at[r])

            @pl.when(has_up)
            def _():
                pass_up(r, plane).start()

            @pl.when(has_down & (r < members - 1))
            def _():
                pass_down(r, plane).start()
            return

        @pl.when(plane >= level)
        def _():
            p = plane - level
            arrived(slot(r, p), kv_recv.at[r, p])

            @pl.when(has_up)
            def _():
                pass_up(r, p).start()

        @pl.when((plane + level < planes) & (r < members - 1))
        def _():
            p = plane + level
            arrived(slot(r, p), kv_recv.at[r, p])

            @pl.when(has_down)
            def _():
                pass_down(r, p).start()

    def advance(t, part):
        r = t + 1 if part == 0 else t - part

        @pl.when((r >= 0) & (r < members))
        def _():
            gather(r, part)

    factor = math.log2(math.e) / math.sqrt(dim)

    def absorb(r, c, masked):
        parts = [kv_buf[c * planes + p] for p in range(planes)]
        looked = jnp.concatenate([part[:, :dim] for part in parts], axis=0)
        values = jnp.concatenate([part[:, dim:] for part in parts], axis=1)
        values = jnp.concatenate([values, jnp.ones((16, keys), jnp.bfloat16)], axis=0)
        if masked:
            t = lax.broadcasted_iota(jnp.int32, (keys, block), 1) + plane * block
            s = lax.broadcasted_iota(jnp.int32, (keys, block), 0)
            allowed = s <= t
        q = jnp.concatenate([q_buf[r, :, g * dim:(g + 1) * dim] for g in range(group)], axis=0)
        scores = lax.dot_general(looked, q, (((1,), (1,)), ((), ())),
                                 preferred_element_type=jnp.float32)
        if masked:
            scores = jnp.where(jnp.concatenate([allowed] * group, axis=1), scores, -1e30)
        old = m_ref[r, :1, :]
        new = jnp.maximum(old, jnp.max(scores, axis=0, keepdims=True))
        m_ref[r, :1, :] = new
        fade = jnp.exp2((old - new) * factor)
        weights = jnp.exp2((scores - new) * factor)
        high = weights.astype(jnp.bfloat16)
        low = (weights - high.astype(jnp.float32)).astype(jnp.bfloat16)
        mixed = jnp.dot(jnp.concatenate([values, values], axis=1),
                        jnp.concatenate([high, low], axis=0),
                        preferred_element_type=jnp.float32)
        acc_ref[r] = acc_ref[r] * fade + mixed

    m_ref[...] = jnp.full_like(m_ref, -1e30)
    acc_ref[...] = jnp.zeros_like(acc_ref)
    gather(0, 0)
    for t in range(planes - 1):
        for part in range(t + 1):
            advance(jnp.int32(t), part)

    half = members // 2

    def one_block(r, carry):
        @pl.when(r <= half)
        def _():
            arrived(q_buf.at[r], q_recv.at[r])

        ahead = jnp.where(r >= 1, jnp.maximum(members - half - r, 0), 0)
        first = jnp.maximum(r - half, 0)
        count = ahead + r - first

        def past(i, carry):
            late = i < ahead
            block_id = jnp.where(late, r + half + i, r)
            chunk = jnp.where(late, r - 1, first + i - ahead)

            @pl.when(late & (r == 1))
            def _():
                arrived(q_buf.at[block_id], q_recv.at[block_id])

            absorb(block_id, chunk, False)
            for level in range(planes):
                @pl.when(i == level)
                def _(level=level):
                    advance(r + planes - 1, level)

            return carry

        lax.fori_loop(0, count, past, 0)
        for level in range(planes):
            @pl.when(level >= count)
            def _(level=level):
                advance(r + planes - 1, level)
        absorb(r, r, True)
        for g in range(group):
            at = pl.ds(g * block, block)
            result = acc_ref[r, :dim, at] / acc_ref[r, dim:dim + 1, at]
            o_buf[r, :, g * dim:(g + 1) * dim] = result.T.astype(jnp.bfloat16)

        @pl.when(r != me)
        def _():
            out_copy(r).start()

        @pl.when(r == me)
        def _():
            pltpu.make_async_copy(o_buf.at[r], out_ref.at[:, lanes(me, wide)],
                                  o_recv.at[me]).start()
        return carry

    lax.fori_loop(0, members, one_block, 0)

    for j in range(1, members):
        k_copy(j).wait_send()
        v_copy(j).wait_send()
        q_copy(j).wait_send()

    def finish(r, carry):
        for p in range(planes):
            @pl.when(has_up & (p <= plane))
            def _(p=p):
                pass_up(r, p).wait_send()

            @pl.when(has_down & (p >= plane) & (r < members - 1))
            def _(p=p):
                pass_down(r, p).wait_send()

        @pl.when(r != me)
        def _():
            out_copy(r).wait_send()

        arrived(out_ref.at[:, lanes(r, wide)], o_recv.at[r])
        return carry

    lax.fori_loop(0, members, finish, 0)


def shards(head_n, inner_n, outer_n, q, k, v):
    block, heads, dim = q.shape
    kv_heads = k.shape[1]
    split = kv_heads // head_n
    assert split * head_n == kv_heads and inner_n % split == 0
    members = kv_heads
    planes = (inner_n // split) * outer_n
    group = heads // kv_heads
    sizes = (head_n, inner_n, outer_n, split, members, planes, block, group, dim)
    rows = group * block
    tokens = members * planes * block
    wide = group * dim
    q2 = q.reshape(block, heads * dim)
    k2 = k.reshape(block, kv_heads * dim)
    v2 = v.transpose(2, 1, 0).reshape(dim, kv_heads * block)
    assert dim == block
    dma = pltpu.SemaphoreType.DMA
    pairs = tokens * rows * planes * members // (2 * members * planes) * members
    out = pl.pallas_call(
        functools.partial(kernel, sizes),
        out_shape=jax.ShapeDtypeStruct((block, heads * dim), jnp.bfloat16),
        in_specs=[pl.BlockSpec(memory_space=pl.ANY)] * 3,
        out_specs=pl.BlockSpec(memory_space=pltpu.VMEM),
        scratch_shapes=[
            pltpu.VMEM((members, block, wide), jnp.bfloat16),
            pltpu.VMEM((members * planes, block, dim + block), jnp.bfloat16),
            pltpu.VMEM((members, block, wide), jnp.bfloat16),
            pltpu.VMEM((members, 8, rows), jnp.float32),
            pltpu.VMEM((members, dim + 16, rows), jnp.float32),
            dma((members,)), dma((members,)),
            dma((members,)), dma((members,)), dma((members,)), dma((members,)),
            dma((members, planes)), dma((members, planes)), dma((members, planes)),
            dma((members,)), dma((members,)),
        ],
        compiler_params=pltpu.CompilerParams(
            collective_id=0, has_side_effects=True, vmem_limit_bytes=2 ** 24 + 16 * tokens * dim),
        cost_estimate=pl.CostEstimate(
            flops=6 * pairs * dim, bytes_accessed=4 * tokens * dim, transcendentals=pairs),
    )(q2, k2, v2)
    return out.reshape(block, heads, dim)


def solution(mesh):
    placed = P(("head", "inner", "outer"), None, None)
    sizes = [mesh.shape[name] for name in ("head", "inner", "outer")]
    return jax.shard_map(
        functools.partial(shards, *sizes),
        mesh=mesh,
        in_specs=(placed, placed, placed),
        out_specs=placed,
        check_vma=False,
    )
```
